32 devices in a mesh: row: 8 (over z, core), col: 4 (over y, x).
Axes of the slice: x: 2, y: 2, z: 4, core: 2. Of those that a mesh axis runs over, the one named last changes fastest.
Arguments:
- gate_input: bfloat16 [2, 512, 53248], P(None, 'col', 'row'), may hold values from -6 to 6
- up_input: bfloat16 [2, 512, 53248], P(None, 'col', 'row'), may hold values from -6 to 6
- down_weight: bfloat16 [53248, 16384], P('row', 'col'), may hold values from -0.02734375 to 0.02734375
Outputs:
- mixed: bfloat16 [2, 512, 16384], P(None, 'row', 'col')
The draws below stay inside these ranges and needn't reach their ends.
All inputs are finite; a program needn't handle non-finite values.
Results may differ from the reference program's by a relative error of at most 0.0049.
Values may be sent and summed in bfloat16 or wider, within the bound.
A program may use at most 128 MiB of HBM per device.

```python
import jax
import jax.numpy as jnp

D = 16384
FF = 53248
SEQS = 2
MINISEQ = 512


def block_scale(key, dims, cuts, least, top_value):
    loudness = 1.0
    for axis_at, blocks in cuts:
        steps = jax.random.uniform(jax.random.fold_in(jax.random.fold_in(key, 6), axis_at), (blocks,), jnp.float32, least / len(cuts), top_value / len(cuts))
        loudness = loudness * jnp.repeat(jnp.exp(steps), dims[axis_at] // blocks).reshape((-1,) + (1,) * (len(dims) - 1 - axis_at))
    return loudness


def centred(own_key, shape, width, most, split=(), dtype=jnp.bfloat16):
    values = width * jax.random.normal(own_key, shape, jnp.float32)
    if split:
        values = values * block_scale(own_key, shape, split, -0.22, 0.18)
    return jnp.clip(values, -most, most).astype(dtype)


def setup_inputs(seed: int = 0) -> dict:
    key_of = jax.random.split(jax.random.key(seed), 4)
    gate_input = centred(key_of[0], (SEQS, MINISEQ, FF), 1.0, 6.0, ((1, 4), (2, 8)))
    up_input = centred(key_of[1], (SEQS, MINISEQ, FF), 1.0, 6.0, ((1, 4), (2, 8)))
    down_weight = centred(key_of[2], (FF, D), FF ** -0.5, 0.02734375, ((0, 8), (1, 4)))
    return dict(gate_input=gate_input, up_input=up_input, down_weight=down_weight)


def reference(gate_input, up_input, down_weight):
    hidden = (jax.nn.silu(gate_input.astype(jnp.float32)) * up_input.astype(jnp.float32)).astype(jnp.bfloat16)
    flat = hidden.reshape(SEQS * MINISEQ, FF)
    mixed = jnp.dot(flat, down_weight, preferred_element_type=jnp.float32)
    return mixed.astype(jnp.bfloat16).reshape(SEQS, MINISEQ, D)
```

```python
import functools

import jax
import jax.numpy as jnp
from jax import lax
from jax.experimental import pallas as pl
from jax.experimental.pallas import tpu as pltpu
from jax.sharding import PartitionSpec as P

MESH = pl.DeviceIdType.MESH
PARTS = 4
AHEAD = 3
LAG = 2
UNIT = 512
ROWS = 16


def gated_hidden(gate_part, up_part):
    product = jax.nn.silu(gate_part.astype(jnp.float32)) * up_part.astype(jnp.float32)
    return product.astype(jnp.bfloat16)


def plan(groups):
    sizes, left = [], groups
    while left:
        take = 2 if left > groups // 2 else 1
        sizes.append(take)
        left -= take
    passes, first = [], 0
    for size in sizes:
        passes.append((first, size))
        first += size
    return passes


def fused(groups, own_ref, w_hbm, out_ref, rem_ref, w, lhs, zrecv, fin, acc, hold, psend, precv, zsend,
          xs, ys, ts, bs, xr, yr, tr, br, ps, pr, zs, zr, ws, ls, osem):
    row, col = lax.axis_index("row"), lax.axis_index("col")
    z, core = row // 2, row % 2
    depth = own_ref.shape[2]
    part = depth // PARTS
    steps = groups * PARTS
    units = w.shape[0]
    xcol = col + 1 - 2 * (col % 2)
    ycol = (col + 2) % 4
    dcol = xcol + 2 - 4 * (xcol // 2)
    cols = [col, xcol, ycol, dcol]

    barrier = pltpu.get_barrier_semaphore()
    peers = [(row, xcol), (row, ycol), (row + 1 - 2 * core, col)]
    peers += [(((z + k) % 4) * 2 + core, col) for k in (1, 2, 3)]
    for peer in peers:
        pl.semaphore_signal(barrier, inc=1, device_id=peer, device_id_type=MESH)
    pl.semaphore_wait(barrier, len(peers))

    def remote(src, dst, send, recv, device):
        return pltpu.make_async_remote_copy(src_ref=src, dst_ref=dst, send_sem=send, recv_sem=recv,
                                            device_id=device, device_id_type=MESH)

    def own_copies(t):
        at = pl.ds((t // PARTS) * 2, 2)
        cut = pl.ds(pl.multiple_of((t % PARTS) * part, 128), part)
        src = own_ref.at[at, :, cut]
        return (remote(src, rem_ref.at[0, at, :, cut], xs.at[t], xr.at[t], (row, xcol)),
                remote(src, rem_ref.at[1, at, :, cut], ys.at[t], yr.at[t], (row, ycol)))

    def relay_copies(t):
        top = (t // PARTS) * 2
        cut = pl.ds(pl.multiple_of((t % PARTS) * part, 128), part)
        return (remote(rem_ref.at[0, top, :, cut], rem_ref.at[2, top, :, cut], ts.at[t], tr.at[t], (row, ycol)),
                remote(rem_ref.at[1, top + 1, :, cut], rem_ref.at[2, top + 1, :, cut], bs.at[t], br.at[t], (row, xcol)))

    def start_own(t):
        for copy in own_copies(t):
            copy.start()

    def gather_step(t):
        for copy in own_copies(t):
            copy.wait_recv()
        for copy in relay_copies(t):
            copy.start()

        @pl.when(t + AHEAD < steps)
        def _():
            start_own(t + AHEAD)

    def w_copy(n):
        return pltpu.make_async_copy(w_hbm.at[:, pl.ds(pl.multiple_of(n * UNIT, 128), UNIT)], w.at[n], ws.at[n])

    pl.loop(0, AHEAD)(start_own)
    own_load = pltpu.make_async_copy(own_ref, lhs, ls.at[0])
    own_load.start()
    pl.loop(0, units)(lambda n: w_copy(n).start())
    own_load.wait()

    mine = jnp.int32(0)
    for j in (1, 2, 3):
        mine = jnp.where(cols[j] == z, j, mine)

    def z_copy(spec, u, n, j, slot):
        base, kinds, first, size = spec
        at = (kinds.index(j)) * size
        to = cols[j]
        sender = (z - to + 3) % 4
        return remote(zsend.at[slot, pl.ds(at, size)], zrecv.at[sender, n, pl.ds(first, size)],
                      zs.at[slot, kinds.index(j)], zr.at[base + n, sender], (to * 2 + core, col))

    def pair_copy(spec, slot):
        _, kinds, _, size = spec
        blocks = len(kinds) * size
        return remote(psend.at[slot, pl.ds(0, blocks)], precv.at[slot, pl.ds(0, blocks)],
                      ps.at[slot], pr.at[slot], (row + 1 - 2 * core, col))

    def z_wait_sent(spec, slot):
        for j in spec[1]:
            @pl.when(mine != j)
            def _():
                z_copy(spec, 0, 0, j, slot).wait_send()

    zslots = zsend.shape[0]

    def combine(spec, before, n):
        _, kinds, first, size = spec
        slot, zslot = n % 2, n % zslots
        pair_copy(spec, slot).wait_recv()
        if before is not None:
            @pl.when(n < zslots)
            def _():
                z_wait_sent(before, zslot)

        @pl.when(n >= zslots)
        def _():
            z_wait_sent(spec, zslot)
        blocks = len(kinds) * size
        for i in range(blocks):
            zsend[zslot, i] = (hold[i] + precv[slot, i].astype(jnp.float32)).astype(zsend.dtype)
        for j in kinds:
            @pl.when(mine == j)
            def _():
                for i in range(size):
                    at = kinds.index(j) * size + i
                    fin[n, first + i] = hold[at] + precv[slot, at].astype(jnp.float32)

            @pl.when(mine != j)
            def _():
                z_copy(spec, 0, n, j, zslot).start()

    def finish(spec):
        base, kinds, first, size = spec

        def one(n):
            for s in range(3):
                pltpu.make_async_copy(zrecv.at[s, n, pl.ds(first, size)], zrecv.at[s, n, pl.ds(first, size)],
                                      zr.at[base + n, s]).wait()
            for i in range(size):
                total = fin[n, first + i]
                for s in range(3):
                    total += zrecv[s, n, first + i].astype(jnp.float32)
                zrecv[0, n, first + i] = total.astype(zrecv.dtype)
            out_copy(spec, n).start()

        @pl.when((mine == 0) if kinds == [0] else (mine != 0))
        def _():
            pl.loop(0, units)(one)

    def out_copy(spec, n):
        base, _, first, size = spec
        return pltpu.make_async_copy(
            zrecv.at[0, n, pl.ds(first, size)],
            out_ref.at[pl.ds(first, size), :, pl.ds(pl.multiple_of(n * UNIT, 128), UNIT)], osem.at[base + n])

    def run_pass(spec, before, block, step, count, wait_w):
        _, kinds, _, size = spec
        blocks = len(kinds) * size
        total = 2 * blocks

        def unit(n):
            if count:
                @pl.when(jnp.logical_and(n % 2 == 0, n // 2 < count))
                def _():
                    gather_step(step + n // 2)
            if wait_w:
                w_copy(n).wait()
            rows = lhs[block:block + total].reshape(total * ROWS, depth)
            acc[0:total] = jnp.dot(rows, w[n], preferred_element_type=jnp.float32).reshape(total, ROWS, UNIT)

            @pl.when(n > 0)
            def _():
                combine(spec, before, n - 1)
            slot = n % 2

            @pl.when(n >= 2)
            def _():
                pair_copy(spec, slot).wait_send()
            for i in range(blocks):
                hold[i] = acc[2 * i + core]
                psend[slot, i] = acc[2 * i + 1 - core].astype(psend.dtype)
            pair_copy(spec, slot).start()

        pl.loop(0, units)(unit)
        combine(spec, before, units - 1)
        for slot in range(2):
            pair_copy(spec, slot).wait_send()

    own_spec = (0, [0], 0, groups)
    during = units // 2
    run_pass(own_spec, None, 0, 0, min(during, steps), True)
    done = min(during, steps)
    before, base, side = own_spec, units, 0
    passes = plan(groups)
    for at, (first, size) in enumerate(passes):
        spec = (base, [1, 2, 3], first, size)
        need = min((first + size) * PARTS + LAG, steps)
        if need > done:
            pl.loop(done, need)(gather_step)
            done = need

        def arrived(t):
            for copy in relay_copies(t):
                copy.wait_recv()
        pl.loop(first * PARTS, (first + size) * PARTS)(arrived)
        block = side * (lhs.shape[0] // 2) if size * 6 <= lhs.shape[0] // 2 else 0
        side = 1 - side
        loads = [pltpu.make_async_copy(rem_ref.at[j, pl.ds(2 * first, 2 * size)],
                                       lhs.at[pl.ds(block + 2 * size * j, 2 * size)], ls.at[j]) for j in range(3)]
        for load in loads:
            load.start()
        for load in loads:
            load.wait()
        count = min(during, steps - done)
        run_pass(spec, before, block, done, count, False)
        done += count
        finish(before)
        before = spec
        base += units
    finish(before)
    for slot in range(zslots):
        z_wait_sent(before, slot)

    def sent(t):
        for copy in own_copies(t) + relay_copies(t):
            copy.wait_send()
    pl.loop(0, steps)(sent)

    specs, base = [own_spec], units
    for first, size in passes:
        specs.append((base, [1, 2, 3], first, size))
        base += units
    for spec in specs:
        @pl.when((mine == 0) if spec[1] == [0] else (mine != 0))
        def _():
            pl.loop(0, units)(lambda n: out_copy(spec, n).wait())


def fused_body(rows, gate_input, up_input, down_weight):
    hidden_units, width = down_weight.shape
    seqs, held, _ = gate_input.shape
    per_core = held // 2
    pieces = per_core // ROWS
    groups = seqs * pieces

    def cut(a):
        a = a.reshape(seqs, 2, pieces, ROWS, hidden_units)
        return a.transpose(0, 2, 1, 3, 4).reshape(2 * groups, ROWS, hidden_units)

    own = gated_hidden(cut(gate_input), cut(up_input))
    units = width // UNIT
    steps = groups * PARTS
    n_units = units * (1 + len(plan(groups)))
    bf16, f32 = jnp.bfloat16, jnp.float32
    dma = pltpu.SemaphoreType.DMA
    hbm = pl.BlockSpec(memory_space=pl.ANY)
    out, _ = pl.pallas_call(
        functools.partial(fused, groups),
        out_shape=[jax.ShapeDtypeStruct((groups, ROWS, width), bf16),
                   jax.ShapeDtypeStruct((3, 2 * groups, ROWS, hidden_units), bf16)],
        in_specs=[hbm, hbm],
        out_specs=[hbm, hbm],
        scratch_shapes=[
            pltpu.VMEM((units, hidden_units, UNIT), bf16),
            pltpu.VMEM((2 * groups, ROWS, hidden_units), bf16),
            pltpu.VMEM((3, units, groups, ROWS, UNIT), bf16),
            pltpu.VMEM((units, groups, ROWS, UNIT), f32),
            pltpu.VMEM((2 * groups, ROWS, UNIT), f32),
            pltpu.VMEM((groups, ROWS, UNIT), f32),
            pltpu.VMEM((2, groups, ROWS, UNIT), bf16),
            pltpu.VMEM((2, groups, ROWS, UNIT), bf16),
            pltpu.VMEM((4, groups, ROWS, UNIT), bf16),
            dma((steps,)), dma((steps,)), dma((steps,)), dma((steps,)),
            dma((steps,)), dma((steps,)), dma((steps,)), dma((steps,)),
            dma((2,)), dma((2,)), dma((4, 3)), dma((n_units, 3)),
            dma((units,)), dma((3,)), dma((n_units,)),
        ],
        compiler_params=pltpu.CompilerParams(collective_id=0, has_side_effects=True, vmem_limit_bytes=67043328),
        cost_estimate=pl.CostEstimate(flops=2 * seqs * held * 4 * hidden_units * width,
                                      bytes_accessed=2 * hidden_units * width, transcendentals=0),
        name="swiglu_down",
    )(own, down_weight)
    return out.reshape(seqs, per_core, width)


def general_body(cols, rows, gate_input, up_input, down_weight):
    hidden_units, _ = down_weight.shape
    seqs, held, _ = gate_input.shape
    flat = lax.all_gather(gated_hidden(gate_input, up_input), "col", axis=1, tiled=True)
    outs = []
    for seq in range(seqs):
        partial_value = jnp.dot(flat[seq], down_weight, preferred_element_type=jnp.float32).astype(jnp.bfloat16)
        outs.append(lax.psum_scatter(partial_value, "row", scatter_dimension=0, tiled=True))
    return jnp.stack(outs, axis=0)


def body(cols, rows, gate_input, up_input, down_weight):
    hidden_units, width = down_weight.shape
    seqs, held, _ = gate_input.shape
    if cols == 4 and rows == 8 and held % (2 * ROWS) == 0 and width % UNIT == 0 and hidden_units % (128 * PARTS) == 0:
        return fused_body(rows, gate_input, up_input, down_weight)
    return general_body(cols, rows, gate_input, up_input, down_weight)


def solution(mesh):
    return jax.shard_map(
        functools.partial(body, mesh.shape["col"], mesh.shape["row"]),
        mesh=mesh,
        in_specs=(P(None, "col", "row"), P(None, "col", "row"), P("row", "col")),
        out_specs=P(None, "row", "col"),
        check_vma=False,
    )
```

```python
import functools

import jax
import jax.numpy as jnp
from jax import lax
from jax.experimental import pallas as pl
from jax.experimental.pallas import tpu as pltpu
from jax.sharding import PartitionSpec as P

MESH = pl.DeviceIdType.MESH
PARTS = 4
AHEAD = 3
LAG = 2
DELAY = 10
GATE = 512
UNIT = 512
ROWS = 16


def gated_hidden(gate_part, up_part):
    product = jax.nn.silu(gate_part.astype(jnp.float32)) * up_part.astype(jnp.float32)
    return product.astype(jnp.bfloat16)


def fused(groups, gate_ref, up_ref, w_hbm, out_ref, rem_ref, w, own, lhs, zrecv, fin, acc, hold, psend, precv, zsend,
          xs, ys, ts, bs, xr, yr, tr, br, ps, pr, zs, zr, ws, ls, gs, osem):
    row, col = lax.axis_index("row"), lax.axis_index("col")
    z, core = row // 2, row % 2
    depth = own.shape[2]
    part = depth // PARTS
    steps = groups * PARTS
    units = w.shape[0]
    total = groups * units
    pieces = gate_ref.shape[2]
    xcol = col + 1 - 2 * (col % 2)
    ycol = (col + 2) % 4
    dcol = xcol + 2 - 4 * (xcol // 2)
    cols = [col, xcol, ycol, dcol]
    partner = (row + 1 - 2 * core, col)

    def load_inputs(g):
        at = 4 * (g % 4)
        seq, piece = g // pieces, g % pieces
        return (pltpu.make_async_copy(gate_ref.at[seq, :, piece], lhs.at[pl.ds(at, 2)], gs.at[g % 4, 0]),
                pltpu.make_async_copy(up_ref.at[seq, :, piece], lhs.at[pl.ds(at + 2, 2)], gs.at[g % 4, 1]))

    def start_load(g):
        for copy in load_inputs(g):
            copy.start()

    pl.loop(0, 4)(start_load)

    barrier = pltpu.get_barrier_semaphore()
    peers = [(row, xcol), (row, ycol), partner]
    peers += [(((z + k) % 4) * 2 + core, col) for k in (1, 2, 3)]
    for peer in peers:
        pl.semaphore_signal(barrier, inc=1, device_id=peer, device_id_type=MESH)
    pl.semaphore_wait(barrier, len(peers))

    def remote(src, dst, send, recv, device):
        return pltpu.make_async_remote_copy(src_ref=src, dst_ref=dst, send_sem=send, recv_sem=recv,
                                            device_id=device, device_id_type=MESH)

    def part_cut(t):
        return pl.ds(pl.multiple_of((t % PARTS) * part, 128), part)

    def own_copies(t):
        at, cut = pl.ds((t // PARTS) * 2, 2), part_cut(t)
        src = own.at[at, :, cut]
        return (remote(src, rem_ref.at[0, at, :, cut], xs.at[t], xr.at[t], (row, xcol)),
                remote(src, rem_ref.at[1, at, :, cut], ys.at[t], yr.at[t], (row, ycol)))

    def relay_copies(t):
        top, cut = (t // PARTS) * 2, part_cut(t)
        return (remote(rem_ref.at[0, top, :, cut], rem_ref.at[2, top, :, cut], ts.at[t], tr.at[t], (row, ycol)),
                remote(rem_ref.at[1, top + 1, :, cut], rem_ref.at[2, top + 1, :, cut], bs.at[t], br.at[t], (row, xcol)))

    def lhs_loads(t):
        g, cut = t // PARTS, part_cut(t)
        return [pltpu.make_async_copy(rem_ref.at[j, pl.ds(2 * g, 2), :, cut],
                                      lhs.at[pl.ds((g % 2) * 8 + 2 * j + 2, 2), :, cut], ls.at[t % (2 * PARTS), j])
                for j in range(3)]

    def start_own(t):
        for copy in own_copies(t):
            copy.start()

    def w_copy(n):
        return pltpu.make_async_copy(w_hbm.at[:, pl.ds(pl.multiple_of(n * UNIT, 128), UNIT)], w.at[n], ws.at[n])

    def gate_group(g):
        for copy in load_inputs(g):
            copy.wait()
        at = 4 * (g % 4)

        def chunk(c):
            cut = pl.ds(pl.multiple_of(c * GATE, 128), GATE)
            for h in range(2):
                v = lhs[at + h, :, cut].astype(jnp.float32)
                u = lhs[at + 2 + h, :, cut].astype(jnp.float32)
                own[2 * g + h, :, cut] = (v / (1.0 + jnp.exp(-v)) * u).astype(own.dtype)
        pl.loop(0, depth // GATE)(chunk)

        @pl.when(g + 4 < groups)
        def _():
            start_load(g + 4)

        @pl.when(g == 0)
        def _():
            pl.loop(0, AHEAD)(start_own)

    pl.loop(0, groups)(gate_group)
    pl.loop(0, units)(lambda n: w_copy(n).start())

    def gather_step(t):
        @pl.when(t < steps)
        def _():
            for copy in own_copies(t):
                copy.wait_recv()
            for copy in relay_copies(t):
                copy.start()

        @pl.when(t + AHEAD < steps)
        def _():
            start_own(t + AHEAD)

        @pl.when(jnp.logical_and(t >= LAG, t < steps + LAG))
        def _():
            for copy in relay_copies(t - LAG):
                copy.wait_recv()
            for copy in lhs_loads(t - LAG):
                copy.start()

    mine = jnp.int32(0)
    for j in (1, 2, 3):
        mine = jnp.where(cols[j] == z, j, mine)
    zslots, fslots = zsend.shape[0], fin.shape[0]

    def z_copy(u, j):
        to = cols[j]
        sender = (z - to + 3) % 4
        return remote(zsend.at[u % zslots, j], zrecv.at[sender, u % units, u // units],
                      zs.at[u % zslots, j], zr.at[u, sender], (to * 2 + core, col))

    def pair_copy(u):
        return remote(psend.at[u % 2], precv.at[u % 2], ps.at[u % 2], pr.at[u % 2], partner)

    def z_wait_sent(u):
        for j in range(4):
            @pl.when(mine != j)
            def _():
                z_copy(u, j).wait_send()

    def combine(u):
        pair_copy(u).wait_recv()

        @pl.when(u >= zslots)
        def _():
            z_wait_sent(u - zslots)
        for j in range(4):
            value = hold[j] + precv[u % 2, j].astype(jnp.float32)
            zsend[u % zslots, j] = value.astype(zsend.dtype)

            @pl.when(mine == j)
            def _():
                fin[u % fslots] = value
        for j in range(4):
            @pl.when(mine != j)
            def _():
                z_copy(u, j).start()

    def out_copy(u):
        n, g = u % units, u // units
        return pltpu.make_async_copy(
            zrecv.at[0, n, g], out_ref.at[g, :, pl.ds(pl.multiple_of(n * UNIT, 128), UNIT)], osem.at[u])

    def finish(u):
        n, g = u % units, u // units
        value = fin[u % fslots]
        for s in range(3):
            pltpu.make_async_copy(zrecv.at[s, n, g], zrecv.at[s, n, g], zr.at[u, s]).wait()
            value += zrecv[s, n, g].astype(jnp.float32)
        zrecv[0, n, g] = value.astype(zrecv.dtype)
        out_copy(u).start()

    def unit(u):
        n, g = u % units, u // units
        side = (g % 2) * 8

        @pl.when(n == 0)
        def _():
            def parts(k):
                for copy in lhs_loads(g * PARTS + k):
                    copy.wait()
            pl.loop(0, PARTS)(parts)
            for h in range(2):
                lhs[side + h] = own[2 * g + h]

        @pl.when(g == 0)
        def _():
            w_copy(n).wait()
        rows = lhs[pl.ds(side, 8)].reshape(8 * ROWS, depth)
        acc[...] = jnp.dot(rows, w[n], preferred_element_type=jnp.float32).reshape(8, ROWS, UNIT)

        @pl.when(u > 0)
        def _():
            combine(u - 1)

        @pl.when(u >= 2)
        def _():
            pair_copy(u - 2).wait_send()
        for j in range(4):
            hold[j] = acc[2 * j + core]
            psend[u % 2, j] = acc[2 * j + 1 - core].astype(psend.dtype)
        pair_copy(u).start()

        @pl.when(u >= DELAY)
        def _():
            finish(u - DELAY)
        per = units // PARTS

        @pl.when(u % per == per - 1)
        def _():
            gather_step(PARTS + LAG + u // per)

    pl.loop(0, PARTS + LAG)(gather_step)
    pl.loop(0, total)(unit)
    combine(total - 1)
    pl.loop(total - DELAY, total)(finish)

    for u in (total - 2, total - 1):
        pair_copy(u).wait_send()
    pl.loop(total - zslots, total)(z_wait_sent)

    def sent(t):
        for copy in own_copies(t) + relay_copies(t):
            copy.wait_send()
    pl.loop(0, steps)(sent)
    pl.loop(0, total)(lambda u: out_copy(u).wait())


def fused_body(gate_input, up_input, down_weight):
    hidden_units, width = down_weight.shape
    seqs, held, _ = gate_input.shape
    per_core = held // 2
    pieces = per_core // ROWS
    groups = seqs * pieces
    units = width // UNIT
    steps = groups * PARTS
    total = groups * units
    bf16, f32 = jnp.bfloat16, jnp.float32
    dma = pltpu.SemaphoreType.DMA
    hbm = pl.BlockSpec(memory_space=pl.ANY)

    def cut(a):
        return a.reshape(seqs, 2, pieces, ROWS, hidden_units)

    out, _ = pl.pallas_call(
        functools.partial(fused, groups),
        out_shape=[jax.ShapeDtypeStruct((groups, ROWS, width), bf16),
                   jax.ShapeDtypeStruct((3, 2 * groups, ROWS, hidden_units), bf16)],
        in_specs=[hbm, hbm, hbm],
        out_specs=[hbm, hbm],
        scratch_shapes=[
            pltpu.VMEM((units, hidden_units, UNIT), bf16),
            pltpu.VMEM((2 * groups, ROWS, hidden_units), bf16),
            pltpu.VMEM((16, ROWS, hidden_units), bf16),
            pltpu.VMEM((3, units, groups, ROWS, UNIT), bf16),
            pltpu.VMEM((16, ROWS, UNIT), f32),
            pltpu.VMEM((8, ROWS, UNIT), f32),
            pltpu.VMEM((4, ROWS, UNIT), f32),
            pltpu.VMEM((2, 4, ROWS, UNIT), bf16),
            pltpu.VMEM((2, 4, ROWS, UNIT), bf16),
            pltpu.VMEM((4, 4, ROWS, UNIT), bf16),
            dma((steps,)), dma((steps,)), dma((steps,)), dma((steps,)),
            dma((steps,)), dma((steps,)), dma((steps,)), dma((steps,)),
            dma((2,)), dma((2,)), dma((4, 4)), dma((total, 3)),
            dma((units,)), dma((2 * PARTS, 3)), dma((4, 2)), dma((total,)),
        ],
        compiler_params=pltpu.CompilerParams(collective_id=0, has_side_effects=True, vmem_limit_bytes=67043328),
        cost_estimate=pl.CostEstimate(flops=2 * seqs * held * 4 * hidden_units * width,
                                      bytes_accessed=2 * hidden_units * width, transcendentals=0),
        name="swiglu_down",
    )(cut(gate_input), cut(up_input), down_weight)
    return out.reshape(seqs, per_core, width)


def general_body(cols, rows, gate_input, up_input, down_weight):
    hidden_units, _ = down_weight.shape
    seqs, held, _ = gate_input.shape
    flat = lax.all_gather(gated_hidden(gate_input, up_input), "col", axis=1, tiled=True)
    outs = []
    for seq in range(seqs):
        partial_value = jnp.dot(flat[seq], down_weight, preferred_element_type=jnp.float32).astype(jnp.bfloat16)
        outs.append(lax.psum_scatter(partial_value, "row", scatter_dimension=0, tiled=True))
    return jnp.stack(outs, axis=0)


def body(cols, rows, gate_input, up_input, down_weight):
    hidden_units, width = down_weight.shape
    seqs, held, _ = gate_input.shape
    if cols == 4 and rows == 8 and held % (2 * ROWS) == 0 and width % UNIT == 0 and hidden_units % GATE == 0 and hidden_units % (128 * PARTS) == 0:
        return fused_body(gate_input, up_input, down_weight)
    return general_body(cols, rows, gate_input, up_input, down_weight)


def solution(mesh):
    return jax.shard_map(
        functools.partial(body, mesh.shape["col"], mesh.shape["row"]),
        mesh=mesh,
        in_specs=(P(None, "col", "row"), P(None, "col", "row"), P("row", "col")),
        out_specs=P(None, "row", "col"),
        check_vma=False,
    )
```

```python
import functools

import jax
import jax.numpy as jnp
from jax import lax
from jax.experimental import pallas as pl
from jax.experimental.pallas import tpu as pltpu
from jax.sharding import PartitionSpec as P

MESH = pl.DeviceIdType.MESH
PARTS = 4
AHEAD = 3
LAG = 2
DELAY = 10
GATE = 512
UNIT = 512
ROWS = 16


def gated_hidden(gate_part, up_part):
    product = jax.nn.silu(gate_part.astype(jnp.float32)) * up_part.astype(jnp.float32)
    return product.astype(jnp.bfloat16)


def fused(groups, gate_ref, up_ref, w_hbm, out_ref, rem_ref, w, own, lhs, zrecv, fin, acc, hold, psend, precv, zsend,
          xs, ys, ts, bs, xr, yr, tr, br, ps, pr, zs, zr, ws, ls, gs, osem):
    row, col = lax.axis_index("row"), lax.axis_index("col")
    z, core = row // 2, row % 2
    depth = own.shape[2]
    part = depth // PARTS
    steps = groups * PARTS
    units = w.shape[0]
    total = groups * units
    pieces = gate_ref.shape[2]
    xcol = col + 1 - 2 * (col % 2)
    ycol = (col + 2) % 4
    dcol = xcol + 2 - 4 * (xcol // 2)
    cols = [col, xcol, ycol, dcol]
    partner = (row + 1 - 2 * core, col)

    def load_inputs(g):
        at = 4 * (g % 4)
        seq, piece = g // pieces, g % pieces
        return (pltpu.make_async_copy(gate_ref.at[seq, :, piece], lhs.at[pl.ds(at, 2)], gs.at[g % 4, 0]),
                pltpu.make_async_copy(up_ref.at[seq, :, piece], lhs.at[pl.ds(at + 2, 2)], gs.at[g % 4, 1]))

    def start_load(g):
        for copy in load_inputs(g):
            copy.start()

    pl.loop(0, 4)(start_load)

    barrier = pltpu.get_barrier_semaphore()
    peers = [(row, xcol), (row, ycol), partner]
    peers += [(((z + k) % 4) * 2 + core, col) for k in (1, 2, 3)]
    for peer in peers:
        pl.semaphore_signal(barrier, inc=1, device_id=peer, device_id_type=MESH)
    pl.semaphore_wait(barrier, len(peers))

    def remote(src, dst, send, recv, device):
        return pltpu.make_async_remote_copy(src_ref=src, dst_ref=dst, send_sem=send, recv_sem=recv,
                                            device_id=device, device_id_type=MESH)

    def part_cut(t):
        return pl.ds(pl.multiple_of((t % PARTS) * part, 128), part)

    def own_copies(t):
        at, cut = pl.ds((t // PARTS) * 2, 2), part_cut(t)
        src = own.at[at, :, cut]
        return (remote(src, rem_ref.at[0, at, :, cut], xs.at[t], xr.at[t], (row, xcol)),
                remote(src, rem_ref.at[1, at, :, cut], ys.at[t], yr.at[t], (row, ycol)))

    def relay_copies(t):
        top, cut = (t // PARTS) * 2, part_cut(t)
        return (remote(rem_ref.at[0, top, :, cut], rem_ref.at[2, top, :, cut], ts.at[t], tr.at[t], (row, ycol)),
                remote(rem_ref.at[1, top + 1, :, cut], rem_ref.at[2, top + 1, :, cut], bs.at[t], br.at[t], (row, xcol)))

    def lhs_loads(t):
        g, cut = t // PARTS, part_cut(t)
        return [pltpu.make_async_copy(rem_ref.at[j, pl.ds(2 * g, 2), :, cut],
                                      lhs.at[pl.ds((g % 2) * 8 + 2 * j + 2, 2), :, cut], ls.at[t % (2 * PARTS), j])
                for j in range(3)]

    def start_own(t):
        for copy in own_copies(t):
            copy.start()

    def w_copy(n):
        return pltpu.make_async_copy(w_hbm.at[:, pl.ds(pl.multiple_of(n * UNIT, 128), UNIT)], w.at[n], ws.at[n])

    def gate_group(g):
        for copy in load_inputs(g):
            copy.wait()
        at = 4 * (g % 4)

        def chunk(c):
            cut = pl.ds(pl.multiple_of(c * GATE, 128), GATE)
            for h in range(2):
                v = lhs[at + h, :, cut].astype(jnp.float32)
                u = lhs[at + 2 + h, :, cut].astype(jnp.float32)
                own[2 * g + h, :, cut] = (v / (1.0 + jnp.exp(-v)) * u).astype(own.dtype)
        pl.loop(0, depth // GATE)(chunk)

        @pl.when(g + 4 < groups)
        def _():
            start_load(g + 4)

        @pl.when(g == 0)
        def _():
            pl.loop(0, AHEAD)(start_own)

    pl.loop(0, groups)(gate_group)
    pl.loop(0, units)(lambda n: w_copy(n).start())

    def gather_step(t):
        @pl.when(t < steps)
        def _():
            for copy in own_copies(t):
                copy.wait_recv()
            for copy in relay_copies(t):
                copy.start()

        @pl.when(t + AHEAD < steps)
        def _():
            start_own(t + AHEAD)

        @pl.when(jnp.logical_and(t >= LAG, t < steps + LAG))
        def _():
            for copy in relay_copies(t - LAG):
                copy.wait_recv()
            for copy in lhs_loads(t - LAG):
                copy.start()

    mine = jnp.int32(0)
    for j in (1, 2, 3):
        mine = jnp.where(cols[j] == z, j, mine)
    end = z // 2 * 3
    far_first = []
    for to in (3 - end, jnp.where(z == end, jnp.where(z == 0, 2, 1), end), jnp.where(z % 3 == 0, jnp.where(z == 0, 1, 2), 3 - z)):
        at = jnp.int32(0)
        for j in (1, 2, 3):
            at = jnp.where(cols[j] == to, j, at)
        far_first.append((to, at))
    zslots, fslots = zsend.shape[0], fin.shape[0]

    def z_copy(u, j):
        to = cols[j]
        sender = (z - to + 3) % 4
        return remote(zsend.at[u % zslots, j], zrecv.at[sender, u % units, u // units],
                      zs.at[u % zslots, j], zr.at[u, sender], (to * 2 + core, col))

    def pair_copy(u):
        return remote(psend.at[u % 2], precv.at[u % 2], ps.at[u % 2], pr.at[u % 2], partner)

    def z_wait_sent(u):
        for j in range(4):
            @pl.when(mine != j)
            def _():
                z_copy(u, j).wait_send()

    def combine(u):
        pair_copy(u).wait_recv()

        @pl.when(u >= zslots)
        def _():
            z_wait_sent(u - zslots)
        for j in range(4):
            value = hold[j] + precv[u % 2, j].astype(jnp.float32)
            zsend[u % zslots, j] = value.astype(zsend.dtype)

            @pl.when(mine == j)
            def _():
                fin[u % fslots] = value
        for to, j in far_first:
            sender = (z - to + 3) % 4
            remote(zsend.at[u % zslots, j], zrecv.at[sender, u % units, u // units],
                   zs.at[u % zslots, j], zr.at[u, sender], (to * 2 + core, col)).start()

    def out_copy(u):
        n, g = u % units, u // units
        return pltpu.make_async_copy(
            zrecv.at[0, n, g], out_ref.at[g, :, pl.ds(pl.multiple_of(n * UNIT, 128), UNIT)], osem.at[u])

    def finish(u):
        n, g = u % units, u // units
        value = fin[u % fslots]
        for s in range(3):
            pltpu.make_async_copy(zrecv.at[s, n, g], zrecv.at[s, n, g], zr.at[u, s]).wait()
            value += zrecv[s, n, g].astype(jnp.float32)
        zrecv[0, n, g] = value.astype(zrecv.dtype)
        out_copy(u).start()

    def unit(u):
        n, g = u % units, u // units
        side = (g % 2) * 8

        @pl.when(n == 0)
        def _():
            def parts(k):
                for copy in lhs_loads(g * PARTS + k):
                    copy.wait()
            pl.loop(0, PARTS)(parts)
            for h in range(2):
                lhs[side + h] = own[2 * g + h]

        @pl.when(g == 0)
        def _():
            w_copy(n).wait()
        rows = lhs[pl.ds(side, 8)].reshape(8 * ROWS, depth)
        acc[...] = jnp.dot(rows, w[n], preferred_element_type=jnp.float32).reshape(8, ROWS, UNIT)

        @pl.when(u > 0)
        def _():
            combine(u - 1)

        @pl.when(u >= 2)
        def _():
            pair_copy(u - 2).wait_send()
        for j in range(4):
            hold[j] = acc[2 * j + core]
            psend[u % 2, j] = acc[2 * j + 1 - core].astype(psend.dtype)
        pair_copy(u).start()

        @pl.when(u >= DELAY)
        def _():
            finish(u - DELAY)
        per = units // PARTS

        @pl.when(u % per == per - 1)
        def _():
            gather_step(PARTS + LAG + u // per)

    pl.loop(0, PARTS + LAG)(gather_step)
    pl.loop(0, total)(unit)
    combine(total - 1)
    pl.loop(total - DELAY, total)(finish)

    for u in (total - 2, total - 1):
        pair_copy(u).wait_send()
    pl.loop(total - zslots, total)(z_wait_sent)

    def sent(t):
        for copy in own_copies(t) + relay_copies(t):
            copy.wait_send()
    pl.loop(0, steps)(sent)
    pl.loop(0, total)(lambda u: out_copy(u).wait())


def fused_body(gate_input, up_input, down_weight):
    hidden_units, width = down_weight.shape
    seqs, held, _ = gate_input.shape
    per_core = held // 2
    pieces = per_core // ROWS
    groups = seqs * pieces
    units = width // UNIT
    steps = groups * PARTS
    total = groups * units
    bf16, f32 = jnp.bfloat16, jnp.float32
    dma = pltpu.SemaphoreType.DMA
    hbm = pl.BlockSpec(memory_space=pl.ANY)

    def cut(a):
        return a.reshape(seqs, 2, pieces, ROWS, hidden_units)

    out, _ = pl.pallas_call(
        functools.partial(fused, groups),
        out_shape=[jax.ShapeDtypeStruct((groups, ROWS, width), bf16),
                   jax.ShapeDtypeStruct((3, 2 * groups, ROWS, hidden_units), bf16)],
        in_specs=[hbm, hbm, hbm],
        out_specs=[hbm, hbm],
        scratch_shapes=[
            pltpu.VMEM((units, hidden_units, UNIT), bf16),
            pltpu.VMEM((2 * groups, ROWS, hidden_units), bf16),
            pltpu.VMEM((16, ROWS, hidden_units), bf16),
            pltpu.VMEM((3, units, groups, ROWS, UNIT), bf16),
            pltpu.VMEM((16, ROWS, UNIT), f32),
            pltpu.VMEM((8, ROWS, UNIT), f32),
            pltpu.VMEM((4, ROWS, UNIT), f32),
            pltpu.VMEM((2, 4, ROWS, UNIT), bf16),
            pltpu.VMEM((2, 4, ROWS, UNIT), bf16),
            pltpu.VMEM((4, 4, ROWS, UNIT), bf16),
            dma((steps,)), dma((steps,)), dma((steps,)), dma((steps,)),
            dma((steps,)), dma((steps,)), dma((steps,)), dma((steps,)),
            dma((2,)), dma((2,)), dma((4, 4)), dma((total, 3)),
            dma((units,)), dma((2 * PARTS, 3)), dma((4, 2)), dma((total,)),
        ],
        compiler_params=pltpu.CompilerParams(collective_id=0, has_side_effects=True, vmem_limit_bytes=67043328),
        cost_estimate=pl.CostEstimate(flops=2 * seqs * held * 4 * hidden_units * width,
                                      bytes_accessed=2 * hidden_units * width, transcendentals=0),
        name="swiglu_down",
    )(cut(gate_input), cut(up_input), down_weight)
    return out.reshape(seqs, per_core, width)


def general_body(cols, rows, gate_input, up_input, down_weight):
    hidden_units, _ = down_weight.shape
    seqs, held, _ = gate_input.shape
    flat = lax.all_gather(gated_hidden(gate_input, up_input), "col", axis=1, tiled=True)
    outs = []
    for seq in range(seqs):
        partial_value = jnp.dot(flat[seq], down_weight, preferred_element_type=jnp.float32).astype(jnp.bfloat16)
        outs.append(lax.psum_scatter(partial_value, "row", scatter_dimension=0, tiled=True))
    return jnp.stack(outs, axis=0)


def body(cols, rows, gate_input, up_input, down_weight):
    hidden_units, width = down_weight.shape
    seqs, held, _ = gate_input.shape
    if cols == 4 and rows == 8 and held % (2 * ROWS) == 0 and width % UNIT == 0 and hidden_units % GATE == 0 and hidden_units % (128 * PARTS) == 0:
        return fused_body(gate_input, up_input, down_weight)
    return general_body(cols, rows, gate_input, up_input, down_weight)


def solution(mesh):
    return jax.shard_map(
        functools.partial(body, mesh.shape["col"], mesh.shape["row"]),
        mesh=mesh,
        in_specs=(P(None, "col", "row"), P(None, "col", "row"), P("row", "col")),
        out_specs=P(None, "row", "col"),
        check_vma=False,
    )
```
